256 devices in a mesh: unit: 4 (over x), replica: 16 (over z, core), model: 4 (over y).
Axes of the slice: x: 4, y: 4, z: 8, core: 2. Of those that a mesh axis runs over, the one named last changes fastest.
Arguments:
- slope_up: float32 [64, 768, 3072], P(('unit', 'replica'), None, 'model'), parts along dimension 0, may hold values from -0.875 to 0.875
- slope_down: float32 [64, 3072, 768], P(('unit', 'replica'), 'model'), parts along dimension 0, may hold values from -0.875 to 0.875
- slope_query: float32 [64, 768, 768], P(('unit', 'replica'), None, 'model'), parts along dimension 0, may hold values from -0.875 to 0.875
- slope_key: float32 [64, 768, 768], P(('unit', 'replica'), None, 'model'), parts along dimension 0, may hold values from -0.875 to 0.875
- slope_value: float32 [64, 768, 768], P(('unit', 'replica'), None, 'model'), parts along dimension 0, may hold values from -0.875 to 0.875
- slope_mixed: float32 [64, 768, 768], P(('unit', 'replica'), 'model'), parts along dimension 0, may hold values from -0.875 to 0.875
- slope_norm: float32 [64, 768], P(('unit', 'replica')), parts along dimension 0, may hold values from -8 to 8
- param_up: float32 [3072, 3072], P(('unit', 'replica'), 'model'), parts along dimension 0, may hold values from -0.21875 to 0.21875
- param_down: float32 [12288, 768], P(('unit', 'model'), 'replica'), parts along dimension 0, may hold values from -0.109375 to 0.109375
- param_query: float32 [3072, 768], P(('unit', 'replica'), 'model'), parts along dimension 0, may hold values from -0.21875 to 0.21875
- param_key: float32 [3072, 768], P(('unit', 'replica'), 'model'), parts along dimension 0, may hold values from -0.21875 to 0.21875
- param_value: float32 [3072, 768], P(('unit', 'replica'), 'model'), parts along dimension 0, may hold values from -0.21875 to 0.21875
- param_mixed: float32 [3072, 768], P(('unit', 'model'), 'replica'), parts along dimension 0, may hold values from -0.21875 to 0.21875
- param_norm: float32 [3072], P(('unit', 'replica')), parts along dimension 0, may hold values from 0.25 to 1.75
Outputs:
- half_up: bfloat16 [3072, 3072], P('unit', 'model'), parts along dimension 0
- half_down: bfloat16 [12288, 768], P(('unit', 'model')), parts along dimension 0
- half_query: bfloat16 [3072, 768], P('unit', 'model'), parts along dimension 0
- half_key: bfloat16 [3072, 768], P('unit', 'model'), parts along dimension 0
- half_value: bfloat16 [3072, 768], P('unit', 'model'), parts along dimension 0
- half_mixed: bfloat16 [3072, 768], P(('unit', 'model')), parts along dimension 0
- half_norm: bfloat16 [3072], P('unit'), parts along dimension 0
- next_up: float32 [3072, 3072], P(('unit', 'replica'), 'model'), parts along dimension 0
- next_down: float32 [12288, 768], P(('unit', 'model'), 'replica'), parts along dimension 0
- next_query: float32 [3072, 768], P(('unit', 'replica'), 'model'), parts along dimension 0
- next_key: float32 [3072, 768], P(('unit', 'replica'), 'model'), parts along dimension 0
- next_value: float32 [3072, 768], P(('unit', 'replica'), 'model'), parts along dimension 0
- next_mixed: float32 [3072, 768], P(('unit', 'model'), 'replica'), parts along dimension 0
- next_norm: float32 [3072], P(('unit', 'replica')), parts along dimension 0
The draws below stay inside these ranges and needn't reach their ends.
There are 4 independent parts, one for each index of `unit`. The reference program is written for one: setup_inputs(seed, part) draws one part's arguments, and reference() takes and returns one part's arrays. A program takes and returns all parts, laid end to end along the dimension named above; each array names one. Nothing has to cross between parts.
All inputs are finite; a program needn't handle non-finite values.
Results may differ from the reference program's by a relative error of at most 0.001.
Values may be sent and summed in bfloat16 or wider, within the bound.
No kernel may reach another device: no remote copies, remote signals or barrier semaphores. Data moves between devices by JAX's collectives and lax.ppermute only.
A program may use at most 64 MiB of HBM per device.

```python
import jax
import jax.numpy as jnp

WIDTH = 768
INNER = 3072
ATTN = 768
REPLICAS = 16


def spiked(array, stream_key, source, target, shards_of, factor):
    owner, partner = [(jnp.arange(array.shape[axis_at]) // (array.shape[axis_at] // shards_of)).reshape([-1 if axis == axis_at else 1 for axis in range(array.ndim)]) for axis_at in (source, target)]
    chosen = jax.random.permutation(stream_key, shards_of)[partner]
    strong = (owner == chosen) | (owner == (partner + shards_of // 2) % shards_of)
    return jnp.where(strong, factor * array, array)


def block_levels(key, shape, split, low, largest):
    gain, own = 1.0, jax.random.fold_in(key, 6)
    for axis_at, parts in split:
        heights = jnp.exp(jax.random.uniform(jax.random.fold_in(own, axis_at), (parts,), jnp.float32, low / len(split), largest / len(split)))
        gain = gain * jnp.repeat(heights, shape[axis_at] // parts).reshape([-1 if axis == axis_at else 1 for axis in range(len(shape))])
    return gain


def centred(stream_key, extent, deviation, reach, split=(), kind=jnp.bfloat16):
    entries = deviation * jax.random.normal(stream_key, extent, jnp.float32)
    if split:
        entries = entries * block_levels(stream_key, extent, split, -0.22, 0.18)
    return jnp.clip(entries, -reach, reach).astype(kind)


def noise_with(stream_key, dims, scale, most, pieces, heavy, dtype=jnp.bfloat16):
    values = scale * jax.random.normal(stream_key, dims, jnp.float32)
    if pieces:
        values = values * block_levels(stream_key, dims, pieces, -0.22, 0.18)
    return jnp.clip(spiked(values, jax.random.fold_in(stream_key, 3), *heavy), -most, most).astype(dtype)


def setup_inputs(seed: int = 0, part: int = 0) -> dict:
    streams_of = jax.random.split(jax.random.key(seed), 15)
    part_keys = jax.random.split(jax.random.fold_in(streams_of[14], part), 15)
    return {
        "slope_up": noise_with(part_keys[0], (REPLICAS, WIDTH, INNER), 0.1, 0.875, ((0, 16), (2, 4)), (0, 1, 16, 2.0), jnp.float32),
        "slope_down": noise_with(part_keys[1], (REPLICAS, INNER, WIDTH), 0.1, 0.875, ((0, 16), (1, 4)), (0, 2, 16, 2.0), jnp.float32),
        "slope_query": noise_with(part_keys[2], (REPLICAS, WIDTH, ATTN), 0.1, 0.875, ((0, 16), (2, 4)), (0, 1, 16, 2.0), jnp.float32),
        "slope_key": noise_with(part_keys[3], (REPLICAS, WIDTH, ATTN), 0.1, 0.875, ((0, 16), (2, 4)), (0, 1, 16, 2.0), jnp.float32),
        "slope_value": noise_with(part_keys[4], (REPLICAS, WIDTH, ATTN), 0.1, 0.875, ((0, 16), (2, 4)), (0, 1, 16, 2.0), jnp.float32),
        "slope_mixed": noise_with(part_keys[5], (REPLICAS, ATTN, WIDTH), 0.1, 0.875, ((0, 16), (1, 4)), (0, 2, 16, 2.0), jnp.float32),
        "slope_norm": noise_with(part_keys[6], (REPLICAS, WIDTH), 1.0, 8.0, ((0, 16),), (0, 1, 16, 2.0), jnp.float32),
        "param_up": centred(part_keys[7], (WIDTH, INNER), WIDTH ** -0.5, 0.21875, ((0, 16), (1, 4)), jnp.float32),
        "param_down": centred(part_keys[8], (INNER, WIDTH), INNER ** -0.5, 0.109375, ((0, 4), (1, 16)), jnp.float32),
        "param_query": centred(part_keys[9], (WIDTH, ATTN), WIDTH ** -0.5, 0.21875, ((0, 16), (1, 4)), jnp.float32),
        "param_key": centred(part_keys[10], (WIDTH, ATTN), WIDTH ** -0.5, 0.21875, ((0, 16), (1, 4)), jnp.float32),
        "param_value": centred(part_keys[11], (WIDTH, ATTN), WIDTH ** -0.5, 0.21875, ((0, 16), (1, 4)), jnp.float32),
        "param_mixed": centred(part_keys[12], (ATTN, WIDTH), ATTN ** -0.5, 0.21875, ((0, 4), (1, 16)), jnp.float32),
        "param_norm": jnp.clip(1.0 + 0.15 * jax.random.normal(part_keys[13], (WIDTH,), jnp.float32), 0.25, 1.75),
    }


learn_rate = 0.3


def reference(slope_up, slope_down, slope_query, slope_key, slope_value, slope_mixed, slope_norm, param_up, param_down, param_query, param_key, param_value, param_mixed, param_norm):
    mean_up = jnp.sum(slope_up.astype(jnp.float32), axis=0) * REPLICAS ** -0.5
    mean_down = jnp.sum(slope_down.astype(jnp.float32), axis=0) * REPLICAS ** -0.5
    mean_query = jnp.sum(slope_query.astype(jnp.float32), axis=0) * REPLICAS ** -0.5
    mean_key = jnp.sum(slope_key.astype(jnp.float32), axis=0) * REPLICAS ** -0.5
    mean_value = jnp.sum(slope_value.astype(jnp.float32), axis=0) * REPLICAS ** -0.5
    mean_mixed = jnp.sum(slope_mixed.astype(jnp.float32), axis=0) * REPLICAS ** -0.5
    mean_norm = jnp.sum(slope_norm.astype(jnp.float32), axis=0) * REPLICAS ** -0.5
    next_up = param_up - learn_rate * mean_up
    next_down = param_down - learn_rate * mean_down
    next_query = param_query - learn_rate * mean_query
    next_key = param_key - learn_rate * mean_key
    next_value = param_value - learn_rate * mean_value
    next_mixed = param_mixed - learn_rate * mean_mixed
    next_norm = param_norm - learn_rate * mean_norm
    half_up = next_up.astype(jnp.bfloat16)
    half_down = next_down.astype(jnp.bfloat16)
    half_query = next_query.astype(jnp.bfloat16)
    half_key = next_key.astype(jnp.bfloat16)
    half_value = next_value.astype(jnp.bfloat16)
    half_mixed = next_mixed.astype(jnp.bfloat16)
    half_norm = next_norm.astype(jnp.bfloat16)
    return half_up, half_down, half_query, half_key, half_value, half_mixed, half_norm, next_up, next_down, next_query, next_key, next_value, next_mixed, next_norm
```

```python
import jax
import jax.numpy as jnp
from jax import lax
from jax.experimental import pallas as pl
from jax.experimental.pallas import tpu as pltpu
from jax.sharding import PartitionSpec as P

learn_rate = 0.3

ROWS = (440, 432)
CUT = 224
GROUPS = ((0, 1, 2, 6, 7), (3, 5), (4,))
f32, bf16 = jnp.float32, jnp.bfloat16
whole = pl.BlockSpec(memory_space=pltpu.VMEM)
scalars = pl.BlockSpec(memory_space=pltpu.SMEM)


def kernel(body, out_shape, in_specs, scratch=()):
    return pl.pallas_call(
        body,
        out_shape=out_shape,
        in_specs=in_specs,
        out_specs=[whole] * len(out_shape),
        scratch_shapes=scratch,
        compiler_params=pltpu.CompilerParams(vmem_limit_bytes=24 << 20),
    )


def three_blocks(a, b):
    tail = jnp.concatenate([a[:, 128:192], b[:, 128:192]], axis=1)
    return a[:, :128], tail, b[:, :128]


def turn(source, target):
    for j in range(6):
        lanes = slice(128 * j, 128 * j + 128)
        target[lanes, :128] = source[0, :128, lanes].T
        rest = jnp.concatenate([source[0, 128:192, lanes], jnp.zeros((64, 128), f32)], axis=0)
        target[lanes, 128:] = rest.T


def chunks(at):
    for k in range(8):
        for shift in (0, 1):
            yield k, shift, 2 * ((at[0] + k) % 8) + (at[1] + shift) % 2


def pack_first_body(at, up, query, key, norm, mine, theirs, q, k_, rows16):
    turn(query, q)
    turn(key, k_)
    rows16[...] = jnp.zeros((16, 128), f32)
    for r in range(16):
        rows16[r : r + 1, :48] = norm[:, 48 * r : 48 * r + 48]
    for k, shift, r in chunks(at):
        out = (mine, theirs)[shift]
        rows = pl.ds(pl.multiple_of(48 * r, 8), 48)
        for j in range(6):
            out[k, 48 * j : 48 * j + 48, :] = up[0, rows, 128 * j : 128 * j + 128]
        for j, block in enumerate(three_blocks(q[rows, :], k_[rows, :])):
            out[k, 288 + 48 * j : 336 + 48 * j, :] = block
        out[k, 432:440, :] = jnp.broadcast_to(rows16[pl.ds(r, 1), :], (8, 128))


def pack_second_body(at, down, value, mixed, mine, theirs, turned, v, m):
    for i in range(6):
        for j in range(6):
            block = down[0, 128 * i : 128 * i + 128, 128 * j : 128 * j + 128]
            turned[128 * j : 128 * j + 128, 128 * i : 128 * i + 128] = block.T
    turn(value, v)
    turn(mixed, m)
    for k, shift, r in chunks(at):
        out = (mine, theirs)[shift]
        rows = pl.ds(pl.multiple_of(48 * r, 8), 48)
        for j in range(6):
            out[k, 48 * j : 48 * j + 48, :] = turned[rows, 128 * j : 128 * j + 128]
        for j, block in enumerate(three_blocks(v[rows, :], m[rows, :])):
            out[k, 288 + 48 * j : 336 + 48 * j, :] = block


def pack_first(at, up, query, key, norm):
    return kernel(
        pack_first_body, [jax.ShapeDtypeStruct((8, 440, 128), f32)] * 2, [scalars] + [whole] * 4,
        [pltpu.VMEM((768, 256), f32)] * 2 + [pltpu.VMEM((16, 128), f32)],
    )(at, up, query, key, norm)


def pack_second(at, down, value, mixed):
    return kernel(
        pack_second_body, [jax.ShapeDtypeStruct((8, 432, 128), f32)] * 2, [scalars] + [whole] * 3,
        [pltpu.VMEM((768, 768), f32)] + [pltpu.VMEM((768, 256), f32)] * 2,
    )(at, down, value, mixed)


def pack_params_body(up, down, query, key, value, mixed, norm, first, second):
    for big, a, b, out in ((up, query, key, first), (down, value, mixed, second)):
        for j in range(6):
            out[48 * j : 48 * j + 48, :] = big[:, 128 * j : 128 * j + 128]
        for j, block in enumerate(three_blocks(a[...], b[...])):
            out[288 + 48 * j : 336 + 48 * j, :] = block
    first[432:440, :] = jnp.zeros((8, 128), f32)
    first[432:433, :48] = norm[...]


def unpack_next_body(first, second, up, down, query, key, value, mixed, norm):
    for new, big, a, b in ((first, up, query, key), (second, down, value, mixed)):
        for j in range(6):
            big[:, 128 * j : 128 * j + 128] = new[48 * j : 48 * j + 48, :]
        tail = new[336:384, :]
        a[:, :128] = new[288:336, :]
        a[:, 128:] = tail[:, :64]
        b[:, :128] = new[384:432, :]
        b[:, 128:] = tail[:, 64:]
    norm[...] = first[432:433, :48]


def pieces(at, refs, rows):
    for shift in (0, 1):
        for ref, ks in zip(refs[3 * shift : 3 * shift + 3], GROUPS):
            for i, k in enumerate(ks):
                r = 2 * ((at[0] + k) % 8) + (at[1] + shift) % 2
                yield r, lambda lo, hi, ref=ref, base=i * rows: ref[base + lo : base + hi, :]


def put_pair(rows, read, a, b):
    first, tail, second = (read(288 + 48 * j, 336 + 48 * j) for j in range(3))
    a[rows, :128] = first
    a[rows, 128:192] = tail[:, :64]
    b[rows, :128] = second
    b[rows, 128:192] = tail[:, 64:]


def turn_back(source, target):
    for j in range(6):
        lanes = slice(128 * j, 128 * j + 128)
        target[:128, lanes] = source[lanes, :128].T
        target[128:, lanes] = source[lanes, 128:].T[:64]


def unpack_first_body(at, *refs):
    up, query, key, norm, q, k_, rows16 = refs[6:]
    for r, read in pieces(at, refs, 440):
        rows = pl.ds(pl.multiple_of(48 * r, 16), 48)
        for j in range(6):
            up[rows, 128 * j : 128 * j + 128] = read(48 * j, 48 * j + 48)
        put_pair(rows, read, q, k_)
        rows16[pl.ds(r, 1), :] = read(432, 440)[:1].astype(f32)
    turn_back(q, query)
    turn_back(k_, key)
    for r in range(16):
        norm[:, 48 * r : 48 * r + 48] = rows16[r : r + 1, :48]


def unpack_second_body(at, *refs):
    down, value, mixed, turned, v, m = refs[6:]
    for r, read in pieces(at, refs, 432):
        rows = pl.ds(pl.multiple_of(48 * r, 16), 48)
        for j in range(6):
            turned[rows, 128 * j : 128 * j + 128] = read(48 * j, 48 * j + 48)
        put_pair(rows, read, v, m)
    for i in range(6):
        for j in range(6):
            block = turned[128 * i : 128 * i + 128, 128 * j : 128 * j + 128]
            down[128 * j : 128 * j + 128, 128 * i : 128 * i + 128] = block.T
    turn_back(v, value)
    turn_back(m, mixed)


def shards(
    slope_up, slope_down, slope_query, slope_key, slope_value, slope_mixed, slope_norm,
    param_up, param_down, param_query, param_key, param_value, param_mixed, param_norm,
):
    n = lax.axis_size("replica")
    chips = n // 2
    me = lax.axis_index("replica")
    at = jnp.stack([me // 2, me % 2]).astype(jnp.int32)
    partner = [(2 * i + k, 2 * i + 1 - k) for i in range(chips) for k in range(2)]
    right = [(2 * i + k, 2 * ((i + 1) % chips) + k) for i in range(chips) for k in range(2)]
    left = [(d, s) for s, d in right]
    rate = learn_rate * n ** (-0.5)
    back = lambda a: jnp.swapaxes(a, -1, -2)

    def send(a, pairs):
        return lax.ppermute(a, "replica", pairs)

    packed = pack_first(at, slope_up, back(slope_query), back(slope_key), slope_norm), pack_second(
        at, slope_down, back(slope_value), slope_mixed
    )
    first, second = kernel(
        pack_params_body, [jax.ShapeDtypeStruct((r, 128), f32) for r in ROWS], [whole] * 7
    )(param_up, back(param_down), param_query, param_key, param_value, back(param_mixed), param_norm.reshape(1, 48))

    news, gots, others = [], [], []
    for (mine, theirs), p in zip(packed, (first, second)):
        pair = send(theirs, partner)
        start = lax.optimization_barrier(mine[4] + pair[4])
        rest = lax.optimization_barrier(tuple(mine[k] + pair[k] for k in range(8) if k != 4))
        own = [*rest[:4], start, *rest[4:]]
        ab = lambda a, b: (send(a, right), send(b, left))
        a, b = ab(own[4][:CUT], own[4][CUT:])
        a = jnp.concatenate([a + own[3][:CUT], own[3][CUT:]])
        b = jnp.concatenate([own[5][:CUT], b + own[5][CUT:]])
        for k in (3, 2, 1):
            a, b = ab(a, b)
            if k > 1:
                a, b = a + own[k - 1], b + own[9 - k]
        new = p - rate * (a + b + own[0])
        news.append(new)
        h = new.astype(bf16)
        got = {0: h}
        a, b = h, h
        for k in range(1, 4):
            a, b = ab(a, b)
            got[8 - k], got[k] = a, b
        got[4] = jnp.concatenate(ab(a[:CUT], b[CUT:]))
        groups = [jnp.concatenate([got[k] for k in ks]) for ks in GROUPS]
        gots.append(groups)
        others.append([send(g, partner) for g in groups])

    shapes = ((48, 768), (48, 768), (48, 192), (48, 192), (48, 192), (48, 192), (1, 48))
    nexts = kernel(unpack_next_body, [jax.ShapeDtypeStruct(x, f32) for x in shapes], [whole] * 2)(*news)
    shape = lambda *x: jax.ShapeDtypeStruct(x, bf16)
    up, query, key, norm = kernel(
        unpack_first_body, [shape(768, 768), shape(192, 768), shape(192, 768), jax.ShapeDtypeStruct((1, 768), f32)],
        [scalars] + [whole] * 6, [pltpu.VMEM((768, 256), bf16)] * 2 + [pltpu.VMEM((16, 128), f32)],
    )(at, *gots[0], *others[0])
    down, value, mixed = kernel(
        unpack_second_body, [shape(768, 768), shape(192, 768), shape(192, 768)],
        [scalars] + [whole] * 6, [pltpu.VMEM((768, 768), bf16)] + [pltpu.VMEM((768, 256), bf16)] * 2,
    )(at, *gots[1], *others[1])
    nup, ndown, nquery, nkey, nvalue, nmixed, nnorm = nexts
    return (
        up, down, back(query), back(key), back(value), mixed, norm.reshape(768).astype(bf16),
        nup, back(ndown), nquery, nkey, nvalue, back(nmixed), nnorm.reshape(48),
    )


def solution(mesh):
    rep = ("unit", "replica")
    um = ("unit", "model")
    args = [P(rep, None, "model"), P(rep, "model", None)] + [P(rep, None, "model")] * 3 + [P(rep, "model", None), P(rep, None)]
    nxt = [P(rep, "model"), P(um, "replica")] + [P(rep, "model")] * 3 + [P(um, "replica"), P(rep)]
    half = [P("unit", "model"), P(um, None)] + [P("unit", "model")] * 3 + [P(um, None), P("unit")]
    return jax.shard_map(shards, mesh=mesh, in_specs=tuple(args + nxt), out_specs=tuple(half + nxt), check_vma=False)
```

```python
import functools

import jax
import jax.numpy as jnp
from jax import lax
from jax.experimental import pallas as pl
from jax.experimental.pallas import tpu as pltpu
from jax.sharding import PartitionSpec as P

learn_rate = 0.3

ROWS = (440, 432)
EARLY, LATE = (4, 5), (0, 1, 2, 3, 6, 7)
GROUPS = ((0, 7, 1), (6, 2), (5, 3), (4,))
f32, bf16 = jnp.float32, jnp.bfloat16
whole = pl.BlockSpec(memory_space=pltpu.VMEM)
scalars = pl.BlockSpec(memory_space=pltpu.SMEM)


def kernel(body, out_shape, in_specs, scratch=()):
    return pl.pallas_call(
        body,
        out_shape=out_shape,
        in_specs=in_specs,
        out_specs=[whole] * len(out_shape),
        scratch_shapes=scratch,
        compiler_params=pltpu.CompilerParams(vmem_limit_bytes=24 << 20),
    )


def three_blocks(a, b):
    tail = jnp.concatenate([a[:, 128:192], b[:, 128:192]], axis=1)
    return a[:, :128], tail, b[:, :128]


def turn(source, target):
    for j in range(6):
        lanes = slice(128 * j, 128 * j + 128)
        target[lanes, :128] = source[0, :128, lanes].T
        rest = jnp.concatenate([source[0, 128:192, lanes], jnp.zeros((64, 128), f32)], axis=0)
        target[lanes, 128:] = rest.T


def chunks(at):
    for k in range(8):
        for shift in (0, 1):
            yield k, shift, 2 * ((at[0] + k) % 8) + (at[1] + shift) % 2


def pack_first_body(at, up_h, query_h, key_h, norm_h, mine, early, late, up, query, key, norm, q, k_, rows16, sems):
    pairs = ((query_h, query), (key_h, key), (norm_h, norm), (up_h, up))
    copies = [pltpu.make_async_copy(x, y, sems.at[i]) for i, (x, y) in enumerate(pairs)]
    for copy in copies:
        copy.start()
    copies[0].wait()
    turn(query, q)
    copies[1].wait()
    turn(key, k_)
    copies[2].wait()
    rows16[...] = jnp.zeros((16, 128), f32)
    for r in range(16):
        rows16[r : r + 1, :48] = norm[:, 48 * r : 48 * r + 48]
    copies[3].wait()
    for k, shift, r in chunks(at):
        out, k = (mine, k) if not shift else (early, k - 4) if k in EARLY else (late, LATE.index(k))
        rows = pl.ds(pl.multiple_of(48 * r, 8), 48)
        for j in range(6):
            out[k, 48 * j : 48 * j + 48, :] = up[0, rows, 128 * j : 128 * j + 128]
        for j, block in enumerate(three_blocks(q[rows, :], k_[rows, :])):
            out[k, 288 + 48 * j : 336 + 48 * j, :] = block
        out[k, 432:440, :] = jnp.broadcast_to(rows16[pl.ds(r, 1), :], (8, 128))


def pack_second_body(at, down, value, mixed, mine, theirs, turned, v, m):
    for i in range(6):
        for j in range(6):
            block = down[0, 128 * i : 128 * i + 128, 128 * j : 128 * j + 128]
            turned[128 * j : 128 * j + 128, 128 * i : 128 * i + 128] = block.T
    turn(value, v)
    turn(mixed, m)
    for k, shift, r in chunks(at):
        out = (mine, theirs)[shift]
        rows = pl.ds(pl.multiple_of(48 * r, 8), 48)
        for j in range(6):
            out[k, 48 * j : 48 * j + 48, :] = turned[rows, 128 * j : 128 * j + 128]
        for j, block in enumerate(three_blocks(v[rows, :], m[rows, :])):
            out[k, 288 + 48 * j : 336 + 48 * j, :] = block


def pack_first(at, up, query, key, norm):
    far = pl.BlockSpec(memory_space=pltpu.HBM)
    return kernel(
        pack_first_body, [jax.ShapeDtypeStruct((n, 440, 128), f32) for n in (8, 2, 6)], [scalars] + [far] * 4,
        [pltpu.VMEM(x.shape, f32) for x in (up, query, key, norm)]
        + [pltpu.VMEM((768, 256), f32)] * 2
        + [pltpu.VMEM((16, 128), f32), pltpu.SemaphoreType.DMA((4,))],
    )(at, *(pltpu.with_memory_space_constraint(x, pltpu.HBM) for x in (up, query, key, norm)))


def pack_second(at, down, value, mixed):
    return kernel(
        pack_second_body, [jax.ShapeDtypeStruct((8, 432, 128), f32)] * 2, [scalars] + [whole] * 3,
        [pltpu.VMEM((768, 768), f32)] + [pltpu.VMEM((768, 256), f32)] * 2,
    )(at, down, value, mixed)


def pack_params_body(up, down, query, key, value, mixed, norm, first, second):
    for big, a, b, out in ((up, query, key, first), (down, value, mixed, second)):
        for j in range(6):
            out[48 * j : 48 * j + 48, :] = big[:, 128 * j : 128 * j + 128]
        for j, block in enumerate(three_blocks(a[...], b[...])):
            out[288 + 48 * j : 336 + 48 * j, :] = block
    first[432:440, :] = jnp.zeros((8, 128), f32)
    first[432:433, :48] = norm[...]


def unpack_next_body(first, second, up, down, query, key, value, mixed, norm):
    for new, big, a, b in ((first, up, query, key), (second, down, value, mixed)):
        for j in range(6):
            big[:, 128 * j : 128 * j + 128] = new[48 * j : 48 * j + 48, :]
        tail = new[336:384, :]
        a[:, :128] = new[288:336, :]
        a[:, 128:] = tail[:, :64]
        b[:, :128] = new[384:432, :]
        b[:, 128:] = tail[:, 64:]
    norm[...] = first[432:433, :48]


def own_chunk(mine, pair, k):
    if pair[0].shape[0] == 8:
        return mine[k] + pair[0][k]
    return mine[k] + (pair[0][k - 4] if k in EARLY else pair[1][LATE.index(k)])


def begin_body(ks, mine, *refs):
    *pair, a, b = refs
    a[...] = own_chunk(mine, pair, ks[0])
    b[...] = own_chunk(mine, pair, ks[1])


def add_body(ks, mine, *refs):
    *pair, got_a, got_b, a, b = refs
    a[...] = got_a[...] + own_chunk(mine, pair, ks[0])
    b[...] = got_b[...] + own_chunk(mine, pair, ks[1])


def add_one_body(k, mine, *refs):
    *pair, got, out = refs
    out[...] = got[...] + own_chunk(mine, pair, k)


def update_body(rate, mine, *refs):
    *pair, got_a, got_b, p, new, half = refs
    value = p[...] - rate * (got_a[...] + got_b[...] + own_chunk(mine, pair, 0))
    new[...] = value
    half[...] = value.astype(bf16)


def join_body(*refs):
    *inputs, out = refs
    at = 0
    for ref in inputs:
        out[at : at + ref.shape[0], :] = ref[...]
        at += ref.shape[0]


def join(arrays):
    rows = sum(a.shape[0] for a in arrays)
    return kernel(join_body, [jax.ShapeDtypeStruct((rows, 128), bf16)], [whole] * len(arrays))(*arrays)[0]


def pieces(at, refs, rows):
    for shift in (0, 1):
        for ref, ks in zip(refs[4 * shift : 4 * shift + 4], GROUPS):
            for i, k in enumerate(ks):
                r = 2 * ((at[0] + k) % 8) + (at[1] + shift) % 2
                yield r, lambda lo, hi, ref=ref, base=i * rows: ref[base + lo : base + hi, :]


def put_pair(rows, read, a, b):
    first, tail, second = (read(288 + 48 * j, 336 + 48 * j) for j in range(3))
    a[rows, :128] = first
    a[rows, 128:192] = tail[:, :64]
    b[rows, :128] = second
    b[rows, 128:192] = tail[:, 64:]


def turn_back(source, target):
    for j in range(6):
        lanes = slice(128 * j, 128 * j + 128)
        target[:128, lanes] = source[lanes, :128].T
        target[128:, lanes] = source[lanes, 128:].T[:64]


def unpack_first_body(at, *refs):
    up, query, key, norm, q, k_, rows16 = refs[8:]
    for r, read in pieces(at, refs, 440):
        rows = pl.ds(pl.multiple_of(48 * r, 16), 48)
        for j in range(6):
            up[rows, 128 * j : 128 * j + 128] = read(48 * j, 48 * j + 48)
        put_pair(rows, read, q, k_)
        rows16[pl.ds(r, 1), :] = read(432, 440)[:1].astype(f32)
    turn_back(q, query)
    turn_back(k_, key)
    for r in range(16):
        norm[:, 48 * r : 48 * r + 48] = rows16[r : r + 1, :48]


def unpack_second_body(at, *refs):
    down, value, mixed, turned, v, m = refs[8:]
    for r, read in pieces(at, refs, 432):
        rows = pl.ds(pl.multiple_of(48 * r, 16), 48)
        for j in range(6):
            turned[rows, 128 * j : 128 * j + 128] = read(48 * j, 48 * j + 48)
        put_pair(rows, read, v, m)
    for i in range(6):
        for j in range(6):
            block = turned[128 * i : 128 * i + 128, 128 * j : 128 * j + 128]
            down[128 * j : 128 * j + 128, 128 * i : 128 * i + 128] = block.T
    turn_back(v, value)
    turn_back(m, mixed)


def shards(
    slope_up, slope_down, slope_query, slope_key, slope_value, slope_mixed, slope_norm,
    param_up, param_down, param_query, param_key, param_value, param_mixed, param_norm,
):
    n = lax.axis_size("replica")
    chips = n // 2
    me = lax.axis_index("replica")
    at = jnp.stack([me // 2, me % 2]).astype(jnp.int32)
    partner = [(2 * i + k, 2 * i + 1 - k) for i in range(chips) for k in range(2)]
    right = [(2 * i + k, 2 * ((i + 1) % chips) + k) for i in range(chips) for k in range(2)]
    left = [(d, s) for s, d in right]
    rate = learn_rate * n ** (-0.5)
    back = lambda a: jnp.swapaxes(a, -1, -2)

    def send(a, pairs):
        return lax.ppermute(a, "replica", pairs)

    mine0, early, late = pack_first(at, slope_up, back(slope_query), back(slope_key), slope_norm)
    early = send(early, partner)
    mine1, theirs1 = pack_second(at, slope_down, back(slope_value), slope_mixed)
    pair0 = send(late, partner)
    pair1 = send(theirs1, partner)
    packed = (mine0, (early, pair0)), (mine1, (pair1,))
    first, second = kernel(
        pack_params_body, [jax.ShapeDtypeStruct((r, 128), f32) for r in ROWS], [whole] * 7
    )(param_up, back(param_down), param_query, param_key, param_value, back(param_mixed), param_norm.reshape(1, 48))

    news, gots, others = [], [], []
    for s, ((mine, pair), p) in enumerate(zip(packed, (first, second))):
        rows = ROWS[s]
        shape = lambda dtype=f32: jax.ShapeDtypeStruct((rows, 128), dtype)
        ab = lambda a, b: (send(a, right), send(b, left))
        known = (mine, *pair)
        specs = [whole] * len(known)
        at_right, at_left = (4, 5) if s == 0 else (3, 4)
        used = 2 if s == 0 else len(known)
        a, b = kernel(functools.partial(begin_body, (at_right, at_left)), [shape()] * 2, specs[:used])(*known[:used])
        for step in range(3):
            a, b = ab(a, b)
            ks = at_right - step - 1, at_left + step + 1
            if step < 2:
                a, b = kernel(functools.partial(add_body, ks), [shape()] * 2, specs + [whole] * 2)(*known, a, b)
        one = kernel(functools.partial(add_one_body, ks[s]), [shape()], specs + [whole])(*known, (a, b)[s])[0]
        one = send(one, (right, left)[s])
        a, b = (one, b) if s == 0 else (a, one)
        new, h = kernel(
            functools.partial(update_body, rate), [shape(), shape(bf16)], specs + [whole] * 3
        )(*known, a, b, p)
        news.append(new)
        a, b = h, h
        groups = []
        for step in range(3):
            a, b = ab(a, b)
            groups.append(join([h, a, b] if step == 0 else [a, b]))
        groups.append(send((a, b)[s], (right, left)[s]))
        gots.append(groups)
        others.append([send(g, partner) for g in groups])

    shapes = ((48, 768), (48, 768), (48, 192), (48, 192), (48, 192), (48, 192), (1, 48))
    nexts = kernel(unpack_next_body, [jax.ShapeDtypeStruct(x, f32) for x in shapes], [whole] * 2)(*news)
    shape = lambda *x: jax.ShapeDtypeStruct(x, bf16)
    up, query, key, norm = kernel(
        unpack_first_body, [shape(768, 768), shape(192, 768), shape(192, 768), jax.ShapeDtypeStruct((1, 768), f32)],
        [scalars] + [whole] * 8, [pltpu.VMEM((768, 256), bf16)] * 2 + [pltpu.VMEM((16, 128), f32)],
    )(at, *gots[0], *others[0])
    down, value, mixed = kernel(
        unpack_second_body, [shape(768, 768), shape(192, 768), shape(192, 768)],
        [scalars] + [whole] * 8, [pltpu.VMEM((768, 768), bf16)] + [pltpu.VMEM((768, 256), bf16)] * 2,
    )(at, *gots[1], *others[1])
    nup, ndown, nquery, nkey, nvalue, nmixed, nnorm = nexts
    return (
        up, down, back(query), back(key), back(value), mixed, norm.reshape(768).astype(bf16),
        nup, back(ndown), nquery, nkey, nvalue, back(nmixed), nnorm.reshape(48),
    )


def solution(mesh):
    rep = ("unit", "replica")
    um = ("unit", "model")
    args = [P(rep, None, "model"), P(rep, "model", None)] + [P(rep, None, "model")] * 3 + [P(rep, "model", None), P(rep, None)]
    nxt = [P(rep, "model"), P(um, "replica")] + [P(rep, "model")] * 3 + [P(um, "replica"), P(rep)]
    half = [P("unit", "model"), P(um, None)] + [P("unit", "model")] * 3 + [P(um, None), P("unit")]
    return jax.shard_map(shards, mesh=mesh, in_specs=tuple(args + nxt), out_specs=tuple(half + nxt), check_vma=False)
```

```python
import functools

import jax
import jax.numpy as jnp
from jax import lax
from jax.experimental import pallas as pl
from jax.experimental.pallas import tpu as pltpu
from jax.sharding import PartitionSpec as P

learn_rate = 0.3

ROWS = (440, 432)
EARLY, LATE = (4, 5), (0, 1, 2, 3, 6, 7)
GROUPS = ((0, 7, 1), (6, 2), (5, 3), (4,))
f32, bf16 = jnp.float32, jnp.bfloat16
whole = pl.BlockSpec(memory_space=pltpu.VMEM)
far = pl.BlockSpec(memory_space=pltpu.HBM)


def kernel(body, out_shape, in_specs, scratch=(), out_specs=None):
    return pl.pallas_call(
        body,
        out_shape=out_shape,
        in_specs=in_specs,
        out_specs=out_specs or [whole] * len(out_shape),
        scratch_shapes=scratch,
        compiler_params=pltpu.CompilerParams(vmem_limit_bytes=24 << 20),
    )


def three_blocks(a, b):
    tail = jnp.concatenate([a[:, 128:192], b[:, 128:192]], axis=1)
    return a[:, :128], tail, b[:, :128]


def turn(source, target):
    for j in range(6):
        lanes = slice(128 * j, 128 * j + 128)
        target[lanes, :128] = source[0, :128, lanes].T
        rest = jnp.concatenate([source[0, 128:192, lanes], jnp.zeros((64, 128), f32)], axis=0)
        target[lanes, 128:] = rest.T


def own_place():
    me = lax.axis_index("replica")
    return lax.div(me, 2), lax.rem(me, 2)


def chunks(at):
    for k in range(8):
        for shift in (0, 1):
            yield k, shift, 2 * ((at[0] + k) % 8) + (at[1] + shift) % 2


def pack_first_body(up_h, query_h, key_h, norm_h, mine, early, late, up, query, key, norm, q, k_, rows16, sems):
    at = own_place()
    pairs = ((query_h, query), (key_h, key), (norm_h, norm), (up_h, up))
    copies = [pltpu.make_async_copy(x, y, sems.at[i]) for i, (x, y) in enumerate(pairs)]
    for copy in copies:
        copy.start()
    copies[0].wait()
    turn(query, q)
    copies[1].wait()
    turn(key, k_)
    copies[2].wait()
    rows16[...] = jnp.zeros((16, 128), f32)
    for r in range(16):
        rows16[r : r + 1, :48] = norm[:, 48 * r : 48 * r + 48]
    copies[3].wait()
    for k, shift, r in chunks(at):
        out, k = (mine, k) if not shift else (early, k - 4) if k in EARLY else (late, LATE.index(k))
        rows = pl.ds(pl.multiple_of(48 * r, 8), 48)
        for j in range(6):
            out[k, 48 * j : 48 * j + 48, :] = up[0, rows, 128 * j : 128 * j + 128]
        for j, block in enumerate(three_blocks(q[rows, :], k_[rows, :])):
            out[k, 288 + 48 * j : 336 + 48 * j, :] = block
        out[k, 432:440, :] = jnp.broadcast_to(rows16[pl.ds(r, 1), :], (8, 128))


def pack_second_body(down, value, mixed, mine, theirs, turned, v, m):
    for i in range(6):
        for j in range(6):
            block = down[0, 128 * i : 128 * i + 128, 128 * j : 128 * j + 128]
            turned[128 * j : 128 * j + 128, 128 * i : 128 * i + 128] = block.T
    turn(value, v)
    turn(mixed, m)
    for k, shift, r in chunks(own_place()):
        out = (mine, theirs)[shift]
        rows = pl.ds(pl.multiple_of(48 * r, 8), 48)
        for j in range(6):
            out[k, 48 * j : 48 * j + 48, :] = turned[rows, 128 * j : 128 * j + 128]
        for j, block in enumerate(three_blocks(v[rows, :], m[rows, :])):
            out[k, 288 + 48 * j : 336 + 48 * j, :] = block


def pack_first(up, query, key, norm):
    return kernel(
        pack_first_body, [jax.ShapeDtypeStruct((n, 440, 128), f32) for n in (8, 2, 6)], [far] * 4,
        [pltpu.VMEM(x.shape, f32) for x in (up, query, key, norm)]
        + [pltpu.VMEM((768, 256), f32)] * 2
        + [pltpu.VMEM((16, 128), f32), pltpu.SemaphoreType.DMA((4,))],
    )(*(pltpu.with_memory_space_constraint(x, pltpu.HBM) for x in (up, query, key, norm)))


def pack_second(down, value, mixed):
    return kernel(
        pack_second_body, [jax.ShapeDtypeStruct((8, 432, 128), f32)] * 2, [whole] * 3,
        [pltpu.VMEM((768, 768), f32)] + [pltpu.VMEM((768, 256), f32)] * 2,
    )(down, value, mixed)


def pack_params_body(up, down, query, key, value, mixed, norm, first, second):
    for big, a, b, out in ((up, query, key, first), (down, value, mixed, second)):
        for j in range(6):
            out[48 * j : 48 * j + 48, :] = big[:, 128 * j : 128 * j + 128]
        for j, block in enumerate(three_blocks(a[...], b[...])):
            out[288 + 48 * j : 336 + 48 * j, :] = block
    first[432:440, :] = jnp.zeros((8, 128), f32)
    first[432:433, :48] = norm[...]


def unpack_next_body(first, second, up, down, query, key, value, mixed, norm):
    for new, big, a, b in ((first, up, query, key), (second, down, value, mixed)):
        for j in range(6):
            big[:, 128 * j : 128 * j + 128] = new[48 * j : 48 * j + 48, :]
        tail = new[336:384, :]
        a[:, :128] = new[288:336, :]
        a[:, 128:] = tail[:, :64]
        b[:, :128] = new[384:432, :]
        b[:, 128:] = tail[:, 64:]
    norm[...] = first[432:433, :48]


def own_chunk(mine, pair, k):
    if pair[0].shape[0] == 8:
        return mine[k] + pair[0][k]
    return mine[k] + (pair[0][k - 4] if k in EARLY else pair[1][LATE.index(k)])


def begin_body(ks, mine, *refs):
    *pair, a, b = refs
    a[...] = own_chunk(mine, pair, ks[0])
    b[...] = own_chunk(mine, pair, ks[1])


def add_body(ks, mine, *refs):
    *pair, got_a, got_b, a, b = refs
    a[...] = got_a[...] + own_chunk(mine, pair, ks[0])
    b[...] = got_b[...] + own_chunk(mine, pair, ks[1])


def add_one_body(k, mine, *refs):
    *pair, got, out = refs
    out[...] = got[...] + own_chunk(mine, pair, k)


def update_body(rate, mine, *refs):
    *pair, got_a, got_b, p, new, half = refs
    value = p[...] - rate * (got_a[...] + got_b[...] + own_chunk(mine, pair, 0))
    new[...] = value
    half[...] = value.astype(bf16)


def join_body(*refs):
    *inputs, out = refs
    at = 0
    for ref in inputs:
        out[at : at + ref.shape[0], :] = ref[...]
        at += ref.shape[0]


def join(arrays):
    rows = sum(a.shape[0] for a in arrays)
    return kernel(join_body, [jax.ShapeDtypeStruct((rows, 128), bf16)], [whole] * len(arrays))(*arrays)[0]


def pieces(at, own, other, groups, rows):
    for shift, refs in ((0, own), (1, other)):
        for ref, ks in zip(refs, groups):
            for i, k in enumerate(ks):
                r = 2 * ((at[0] + k) % 8) + (at[1] + shift) % 2
                yield r, lambda lo, hi, ref=ref, base=i * rows: ref[base + lo : base + hi, :]


def put_pair(rows, read, a, b):
    first, tail, second = (read(288 + 48 * j, 336 + 48 * j) for j in range(3))
    a[rows, :128] = first
    a[rows, 128:192] = tail[:, :64]
    b[rows, :128] = second
    b[rows, 128:192] = tail[:, 64:]


def turn_back(source, target):
    for j in range(6):
        lanes = slice(128 * j, 128 * j + 128)
        target[:128, lanes] = source[lanes, :128].T
        target[128:, lanes] = source[lanes, 128:].T[:64]


def put_first(at, own, other, groups, up, q, k_, rows16):
    for r, read in pieces(at, own, other, groups, 440):
        rows = pl.ds(pl.multiple_of(48 * r, 16), 48)
        for j in range(6):
            up[rows, 128 * j : 128 * j + 128] = read(48 * j, 48 * j + 48)
        put_pair(rows, read, q, k_)
        rows16[pl.ds(r, 1), :] = read(432, 440)[:1].astype(f32)


def open_first_body(*refs):
    put_first(own_place(), refs[:3], refs[3:6], GROUPS[:3], *refs[6:])


def unpack_first_body(
    own, other, up_in, q_in, k_in, rows_in, up_h, query_h, key_h, norm, up, query, key, q, k_, rows16, sems
):
    copies = [
        pltpu.make_async_copy(x, y, sems.at[i]) for i, (x, y) in enumerate(((up, up_h), (query, query_h), (key, key_h)))
    ]
    up[...] = up_in[...]
    q[...] = q_in[...]
    k_[...] = k_in[...]
    rows16[...] = rows_in[...]
    put_first(own_place(), (own,), (other,), GROUPS[3:], up, q, k_, rows16)
    copies[0].start()
    turn_back(q, query)
    copies[1].start()
    turn_back(k_, key)
    copies[2].start()
    for r in range(16):
        norm[:, 48 * r : 48 * r + 48] = rows16[r : r + 1, :48]
    for copy in copies:
        copy.wait()


def unpack_second_body(*refs):
    down_h, value_h, mixed_h, down, value, mixed, turned, v, m, sems = refs[8:]
    for r, read in pieces(own_place(), refs[:4], refs[4:8], GROUPS, 432):
        rows = pl.ds(pl.multiple_of(48 * r, 16), 48)
        for j in range(6):
            turned[rows, 128 * j : 128 * j + 128] = read(48 * j, 48 * j + 48)
        put_pair(rows, read, v, m)
    copies = [
        pltpu.make_async_copy(down.at[pl.ds(128 * j, 128), :], down_h.at[pl.ds(128 * j, 128), :], sems.at[j])
        for j in range(6)
    ]
    copies += [pltpu.make_async_copy(value, value_h, sems.at[6]), pltpu.make_async_copy(mixed, mixed_h, sems.at[7])]
    turn_back(v, value)
    copies[6].start()
    turn_back(m, mixed)
    copies[7].start()
    for j in range(6):
        for i in range(6):
            block = turned[128 * i : 128 * i + 128, 128 * j : 128 * j + 128]
            down[128 * j : 128 * j + 128, 128 * i : 128 * i + 128] = block.T
        copies[j].start()
    for copy in copies:
        copy.wait()


def shards(
    slope_up, slope_down, slope_query, slope_key, slope_value, slope_mixed, slope_norm,
    param_up, param_down, param_query, param_key, param_value, param_mixed, param_norm,
):
    n = lax.axis_size("replica")
    chips = n // 2
    partner = [(2 * i + k, 2 * i + 1 - k) for i in range(chips) for k in range(2)]
    right = [(2 * i + k, 2 * ((i + 1) % chips) + k) for i in range(chips) for k in range(2)]
    left = [(d, s) for s, d in right]
    rate = learn_rate * n ** (-0.5)
    back = lambda a: jnp.swapaxes(a, -1, -2)

    def send(a, pairs):
        return lax.ppermute(a, "replica", pairs)

    mine0, early, late = pack_first(slope_up, back(slope_query), back(slope_key), slope_norm)
    early = send(early, partner)
    mine1, theirs1 = pack_second(slope_down, back(slope_value), slope_mixed)
    pair0 = send(late, partner)
    pair1 = send(theirs1, partner)
    packed = (mine0, (early, pair0)), (mine1, (pair1,))
    first, second = kernel(
        pack_params_body, [jax.ShapeDtypeStruct((r, 128), f32) for r in ROWS], [whole] * 7
    )(param_up, back(param_down), param_query, param_key, param_value, back(param_mixed), param_norm.reshape(1, 48))

    news, gots, others = [], [], []
    for s, ((mine, pair), p) in enumerate(zip(packed, (first, second))):
        rows = ROWS[s]
        shape = lambda dtype=f32: jax.ShapeDtypeStruct((rows, 128), dtype)
        ab = lambda a, b: (send(a, right), send(b, left))
        known = (mine, *pair)
        specs = [whole] * len(known)
        at_right, at_left = (4, 5) if s == 0 else (3, 4)
        used = 2 if s == 0 else len(known)
        a, b = kernel(functools.partial(begin_body, (at_right, at_left)), [shape()] * 2, specs[:used])(*known[:used])
        for step in range(3):
            a, b = ab(a, b)
            ks = at_right - step - 1, at_left + step + 1
            if step < 2:
                a, b = kernel(functools.partial(add_body, ks), [shape()] * 2, specs + [whole] * 2)(*known, a, b)
        one = kernel(functools.partial(add_one_body, ks[s]), [shape()], specs + [whole])(*known, (a, b)[s])[0]
        one = send(one, (right, left)[s])
        a, b = (one, b) if s == 0 else (a, one)
        new, h = kernel(
            functools.partial(update_body, rate), [shape(), shape(bf16)], specs + [whole] * 3
        )(*known, a, b, p)
        news.append(new)
        a, b = h, h
        groups = []
        for step in range(3):
            a, b = ab(a, b)
            groups.append(join([h, a, b] if step == 0 else [a, b]))
        groups.append(send((a, b)[s], (right, left)[s]))
        gots.append(groups)
        others.append([send(g, partner) for g in groups])

    shapes = ((48, 768), (48, 768), (48, 192), (48, 192), (48, 192), (48, 192), (1, 48))
    nexts = kernel(unpack_next_body, [jax.ShapeDtypeStruct(x, f32) for x in shapes], [whole] * 2)(*news)
    shape = lambda *x: jax.ShapeDtypeStruct(x, bf16)
    wide, row = shape(768, 256), jax.ShapeDtypeStruct((16, 128), f32)
    opened = kernel(open_first_body, [shape(768, 768), wide, wide, row], [whole] * 6)(*gots[0][:3], *others[0][:3])
    up, query, key, norm = kernel(
        unpack_first_body, [shape(768, 768), shape(192, 768), shape(192, 768), jax.ShapeDtypeStruct((1, 768), f32)],
        [whole] * 6, [pltpu.VMEM((768, 768), bf16)] + [pltpu.VMEM((192, 768), bf16)] * 2 + [pltpu.VMEM((768, 256), bf16)] * 2
        + [pltpu.VMEM((16, 128), f32), pltpu.SemaphoreType.DMA((3,))], [far] * 3 + [whole],
    )(gots[0][3], others[0][3], *opened)
    down, value, mixed = kernel(
        unpack_second_body, [shape(768, 768), shape(192, 768), shape(192, 768)],
        [whole] * 8, [pltpu.VMEM((768, 768), bf16)] + [pltpu.VMEM((192, 768), bf16)] * 2 + [pltpu.VMEM((768, 768), bf16)]
        + [pltpu.VMEM((768, 256), bf16)] * 2 + [pltpu.SemaphoreType.DMA((8,))], [far] * 3,
    )(*gots[1], *others[1])
    nup, ndown, nquery, nkey, nvalue, nmixed, nnorm = nexts
    return (
        up, down, back(query), back(key), back(value), mixed, norm.reshape(768).astype(bf16),
        nup, back(ndown), nquery, nkey, nvalue, back(nmixed), nnorm.reshape(48),
    )


def solution(mesh):
    rep = ("unit", "replica")
    um = ("unit", "model")
    args = [P(rep, None, "model"), P(rep, "model", None)] + [P(rep, None, "model")] * 3 + [P(rep, "model", None), P(rep, None)]
    nxt = [P(rep, "model"), P(um, "replica")] + [P(rep, "model")] * 3 + [P(um, "replica"), P(rep)]
    half = [P("unit", "model"), P(um, None)] + [P("unit", "model")] * 3 + [P(um, None), P("unit")]
    return jax.shard_map(shards, mesh=mesh, in_specs=tuple(args + nxt), out_specs=tuple(half + nxt), check_vma=False)
```
